32 devices in a mesh: intra: 4 (over y, x), inter: 8 (over z, core).
Axes of the slice: x: 2, y: 2, z: 4, core: 2. Of those that a mesh axis runs over, the one named last changes fastest.
Arguments:
- gate_pre: bfloat16 [1536, 14336], P('intra', 'inter'), may hold values from -6 to 6
- up_pre: bfloat16 [1536, 14336], P('intra', 'inter'), may hold values from -6 to 6
- cotangent: bfloat16 [1536, 8192], P('intra'), may hold values from -6 to 6
- weight_codes: bfloat16 [8192, 14336], P('intra', 'inter'), may hold values from -0.0625 to 0.0625
- weight_scale: bfloat16 [128, 14336], P('intra', 'inter'), may hold values from 0.5 to 2
- section_one: float32 [128, 14336], P(None, 'inter'), may hold values from 1 to 20
- section_two: float32 [128, 14336], P('intra', 'inter'), may hold values from 4 to 60
Outputs:
- grad_gate: bfloat16 [1536, 14336], P('intra', 'inter')
- grad_up: bfloat16 [1536, 14336], P('intra', 'inter')
- grad_codes: float32 [8192, 14336], P(('intra', 'inter'))
The draws below stay inside these ranges and needn't reach their ends.
All inputs are finite; a program needn't handle non-finite values.
Results may differ from the reference program's by a relative error of at most 0.015.
Values may be sent and summed in bfloat16 or wider, within the bound.
A program may use at most 256 MiB of HBM per device.

```python
import math
import jax
import jax.numpy as jnp
from jax import lax

D = 8192
FW = 14336
BLK = 64
TOK_DEV = 384
TOKENS = 1536
NB = 128
N_INTRA = 4


def block_levels(stream_key, dims, shards, smallest, high):
    def one(dim, shards_of):
        steps = jax.random.uniform(jax.random.fold_in(jax.random.fold_in(stream_key, 6), dim), (shards_of,), jnp.float32, smallest / len(shards), high / len(shards))
        return jnp.repeat(jnp.exp(steps), dims[dim] // shards_of).reshape((-1,) + (1,) * (len(dims) - dim - 1))

    factor_of = one(*shards[0])
    for cut in shards[1:]:
        factor_of = factor_of * one(*cut)
    return factor_of


def bell_draw(stream_key, shape, width, bound, split=(), kind=jnp.bfloat16):
    entries = width * jax.random.normal(stream_key, shape, jnp.float32)
    if split:
        entries = entries * block_levels(stream_key, shape, split, -0.22, 0.18)
    return jnp.clip(entries, -bound, bound).astype(kind)


def setup_inputs(seed: int = 0) -> dict:
    streams_of = jax.random.split(jax.random.key(seed), 8)
    return {
        "gate_pre": bell_draw(streams_of[0], (TOKENS, FW), 1.0, 6.0, ((0, 4), (1, 8))),
        "up_pre": bell_draw(streams_of[1], (TOKENS, FW), 1.0, 6.0, ((0, 4), (1, 8))),
        "cotangent": bell_draw(streams_of[2], (TOKENS, D), 1.0, 6.0, ((0, 4),)),
        "weight_codes": bell_draw(streams_of[3], (D, FW), D ** -0.5, 0.0625, ((0, 4), (1, 8))),
        "weight_scale": jnp.clip(jnp.exp(math.log(2.0) - 1.3862944 * jax.random.uniform(streams_of[4], (NB, FW), jnp.float32) ** block_levels(streams_of[4], (NB, FW), ((0, 4), (1, 8)), -0.2, 0.2)), 0.5, 2.0).astype(jnp.bfloat16),
        "section_one": jnp.clip(jnp.exp(math.log(20.0) - 2.9957323 * jax.random.uniform(streams_of[5], (NB, FW), jnp.float32) ** block_levels(streams_of[5], (NB, FW), ((1, 8),), -0.2, 0.2)), 1.0, 20.0),
        "section_two": jnp.clip(jnp.exp(math.log(60.0) - 2.7080502 * jax.random.uniform(streams_of[6], (NB, FW), jnp.float32) ** block_levels(streams_of[6], (NB, FW), ((0, 4), (1, 8)), -0.2, 0.2)), 4.0, 60.0),
    }


def soft_code(values):
    return 7.0 * jnp.tanh(values / 7.0)


def expand(scales):
    return jnp.repeat(scales, BLK, axis=0)


def reference(gate_pre, up_pre, cotangent, weight_codes, weight_scale, section_one, section_two):
    layer = (weight_codes.astype(jnp.float32) * expand(weight_scale).astype(jnp.float32)).astype(jnp.bfloat16)
    one_full = expand(section_one)
    two_full = expand(section_two)

    def block_step(total, block_index):
        start = (block_index * TOK_DEV).astype(jnp.int32)
        rows_out = lax.dynamic_slice_in_dim(cotangent, start, TOK_DEV, 0)
        gate_rows = lax.dynamic_slice_in_dim(gate_pre, start, TOK_DEV, 0).astype(jnp.float32)
        up_rows = lax.dynamic_slice_in_dim(up_pre, start, TOK_DEV, 0).astype(jnp.float32)
        sigma = jax.nn.sigmoid(gate_rows)
        gated = gate_rows * sigma
        hidden = (gated * up_rows).astype(jnp.bfloat16)
        grad_hidden = jnp.dot(rows_out, layer, preferred_element_type=jnp.float32)
        grad_gate = (grad_hidden * up_rows * sigma * (1.0 + gate_rows * (1.0 - sigma))).astype(jnp.bfloat16)
        grad_up = (grad_hidden * gated).astype(jnp.bfloat16)
        term = jnp.dot(rows_out.T, hidden, preferred_element_type=jnp.float32)
        coded = lax.optimization_barrier(soft_code(term / one_full).astype(jnp.bfloat16))
        return total + coded.astype(jnp.float32), (grad_gate, grad_up)

    first, grads = lax.scan(block_step, jnp.zeros((D, FW), jnp.float32), jnp.arange(N_INTRA, dtype=jnp.int32))
    second = soft_code(first * one_full / two_full).astype(jnp.bfloat16).astype(jnp.float32)
    grad_gate = grads[0].reshape(TOK_DEV * N_INTRA, FW)
    grad_up = grads[1].reshape(TOK_DEV * N_INTRA, FW)
    return grad_gate, grad_up, second
```

```python
import functools

import jax
import jax.numpy as jnp
from jax import lax
from jax.experimental import pallas as pl
from jax.experimental.pallas import tpu as pltpu
from jax.sharding import PartitionSpec as P


def code_rows(blk, cols_ref, hidden_ref, one_ref, two_ref, out_ref):
    groups, tok, rows = cols_ref.shape
    total = [None] * (rows // blk)
    for a in range(groups):
        term = lax.dot_general(
            cols_ref[a], hidden_ref[a * tok:(a + 1) * tok, :], (((0,), (0,)), ((), ())),
            preferred_element_type=jnp.float32,
        )
        for b in range(rows // blk):
            coded = jnp.tanh(term[b * blk:(b + 1) * blk] * (1.0 / (7.0 * one_ref[b])))
            total[b] = coded if a == 0 else total[b] + coded
    for b in range(rows // blk):
        second = 7.0 * jnp.tanh(total[b] * (one_ref[b] / two_ref[b]))
        out_ref[b * blk:(b + 1) * blk, :] = second.astype(out_ref.dtype)


def recoded_rows(cols, hidden, one, two, blk):
    groups, tok, rows = cols.shape
    width = hidden.shape[1]
    tile = min(256, rows)
    scale_spec = pl.BlockSpec((tile // blk, 1, width), lambda i: (i, 0, 0))
    return pl.pallas_call(
        functools.partial(code_rows, blk),
        grid=(rows // tile,),
        in_specs=[
            pl.BlockSpec((groups, tok, tile), lambda i: (0, 0, i)),
            pl.BlockSpec((groups * tok, width), lambda i: (0, 0)),
            scale_spec,
            scale_spec,
        ],
        out_specs=pl.BlockSpec((tile, width), lambda i: (i, 0)),
        out_shape=jax.ShapeDtypeStruct((rows, width), jnp.bfloat16),
        cost_estimate=pl.CostEstimate(
            flops=2 * rows * width * groups * tok,
            bytes_accessed=2 * (cols.size + hidden.size + rows * width),
            transcendentals=(groups + 1) * rows * width,
        ),
        compiler_params=pltpu.CompilerParams(vmem_limit_bytes=40 * 2**20),
    )(cols, hidden, one, two)


def join_rows(*refs):
    start = 0
    for ref in refs[:-1]:
        refs[-1][:, start:start + ref.shape[1]] = ref[...].astype(jnp.float32)
        start += ref.shape[1]


def joined_rows(owned):
    sources, rows, _ = owned[0].shape
    width = sum(p.shape[2] for p in owned)
    return pl.pallas_call(
        join_rows,
        grid=(sources,),
        in_specs=[pl.BlockSpec((None, rows, p.shape[2]), lambda j: (j, 0, 0)) for p in owned],
        out_specs=pl.BlockSpec((rows, width), lambda j: (0, j)),
        out_shape=jax.ShapeDtypeStruct((rows, sources * width), jnp.float32),
        cost_estimate=pl.CostEstimate(
            flops=0, bytes_accessed=6 * sources * rows * width, transcendentals=0
        ),
        compiler_params=pltpu.CompilerParams(vmem_limit_bytes=24 * 2**20),
    )(*owned)


def on_device(gate_pre, up_pre, cotangent, weight_codes, weight_scale, section_one, section_two):
    width = weight_codes.shape[1]
    n_blocks = weight_scale.shape[0]
    blk = weight_codes.shape[0] // n_blocks
    n_intra = lax.axis_size("intra")
    n_inter = lax.axis_size("inter")
    own_rows = cotangent.shape[1] // n_intra
    tok = cotangent.shape[0]
    core = lax.axis_index("inter") % 2

    half = lax.dynamic_slice_in_dim(cotangent, core * (tok // 2), tok // 2, 0)
    mine = lax.all_to_all(
        half.reshape(tok // 2, n_intra, own_rows).transpose(1, 0, 2), "intra", 0, 0
    )
    other = lax.ppermute(mine, "inter", [(i, i ^ 1) for i in range(n_inter)])
    cols = jnp.concatenate(
        [jnp.where(core == 0, mine, other), jnp.where(core == 0, other, mine)], axis=1
    )

    gate_rows = gate_pre.astype(jnp.float32)
    up_rows = up_pre.astype(jnp.float32)
    sigma = jax.nn.sigmoid(gate_rows)
    gated = gate_rows * sigma
    hidden = (gated * up_rows).astype(jnp.bfloat16)
    one = lax.dynamic_slice_in_dim(
        section_one, lax.axis_index("intra") * n_blocks, n_blocks, 0
    ).reshape(n_blocks, 1, width)
    two = section_two.reshape(n_blocks, 1, width)

    cut = width // 128 * 3 // 7 * 128
    spans = [(0, cut), (cut, width)] if cut else [(0, width)]
    gathered = []
    piece = hidden
    for lo, hi in spans:
        piece = hidden[:, lo:hi]
        if gathered:
            piece, gathered[-1] = lax.optimization_barrier((piece, gathered[-1]))
        gathered.append(lax.all_gather(piece, "intra", axis=0, tiled=True))

    pieces = []
    for (lo, hi), full in zip(spans, gathered):
        pieces.append(recoded_rows(cols, full, one[:, :, lo:hi], two[:, :, lo:hi], blk))
        if len(pieces) == 1:
            pieces[0], late_cols = lax.optimization_barrier((pieces[0], cols))

    own_layer = (
        weight_codes.reshape(n_blocks, blk, width).astype(jnp.float32)
        * weight_scale.astype(jnp.float32)[:, None, :]
    ).astype(jnp.bfloat16).reshape(-1, width)
    partial_rows = jnp.dot(
        late_cols.reshape(n_intra * tok, own_rows), own_layer, preferred_element_type=jnp.float32
    ).astype(jnp.bfloat16)
    partial_rows, _ = lax.optimization_barrier((partial_rows, gathered[-1]))
    grad_hidden = lax.psum_scatter(
        partial_rows, "intra", scatter_dimension=0, tiled=True
    ).astype(jnp.float32)
    grad_gate = (grad_hidden * up_rows * sigma * (1.0 + gate_rows * (1.0 - sigma))).astype(
        jnp.bfloat16
    )
    grad_up = (grad_hidden * gated).astype(jnp.bfloat16)

    owned = [
        lax.all_to_all(
            p.reshape(n_inter, own_rows // n_inter, p.shape[1]), "inter", 0, 0
        )
        for p in pieces
    ]
    return (grad_gate, grad_up, joined_rows(owned))


def solution(mesh):
    placed = (
        P("intra", "inter"),
        P("intra", "inter"),
        P("intra", None),
        P("intra", "inter"),
        P("intra", "inter"),
        P(None, "inter"),
        P("intra", "inter"),
    )
    return jax.shard_map(
        on_device,
        mesh=mesh,
        in_specs=placed,
        out_specs=(P("intra", "inter"), P("intra", "inter"), P(("intra", "inter"), None)),
        check_vma=False,
    )
```
